32 devices in a mesh: dp: 8 (over y, x, core), tm: 4 (over z).
Axes of the slice: x: 2, y: 2, z: 4, core: 2. Of those that a mesh axis runs over, the one named last changes fastest.
Arguments:
- tokens: bfloat16 [8, 4, 256, 1024], P('dp', 'tm'), may hold values from -6 to 6
- gain: bfloat16 [1024], replicated, may hold values from 0.25 to 1.75
- w_qkv: bfloat16 [1024, 3072], P('dp'), may hold values from -0.1875 to 0.1875
- w_out: bfloat16 [1024, 1024], P('dp'), may hold values from -0.1875 to 0.1875
- w_pair: float32 [2, 1024, 32], replicated, may hold values from -3 to 3
- codebook: float32 [8, 32], replicated, may hold values from -5 to 5
- codes: int32 [8, 4, 1], P('dp', 'tm'), may hold values from 0 to 7
Outputs:
- grad_tokens: bfloat16 [8, 4, 256, 1024], P('dp', 'tm')
- grad_pair: float32 [2, 1024, 32], replicated
- codebook_step: float32 [8, 32], replicated
The draws below stay inside these ranges and needn't reach their ends.
Inputs may be any that keep to these rules, and one draw needn't show every extreme that they name: Every one of the 8 codes is assigned to some clip frame.
All inputs are finite; a program needn't handle non-finite values.
Results may differ from the reference program's by a relative error of at most 0.014.
Values may be sent and summed in bfloat16 or wider, within the bound.
A program may use at most 64 MiB of HBM per device.

```python
import jax
import jax.numpy as jnp
from jax import lax

D = 1024
HEAD_DIM = 64
LATENT = 32
CODES = 8
PATCHES = 256
CLIPS = 8
FRAMES = 4


def levels(rng, dims, pieces, least, top_value):
    loudness, own = 1.0, jax.random.fold_in(rng, 6)
    for dim, blocks in pieces:
        heights = jnp.exp(jax.random.uniform(jax.random.fold_in(own, dim), (blocks,), jnp.float32, least / len(pieces), top_value / len(pieces)))
        loudness = loudness * jnp.repeat(heights, dims[dim] // blocks).reshape([-1 if axis == dim else 1 for axis in range(len(dims))])
    return loudness


def distinct(key, rows, number_of, top, lift):
    ranking = jax.random.permutation(jax.random.fold_in(key, 1), number_of)
    favour = ranking
    for power in range(3):
        favour = favour * favour // number_of
    favour = favour * lift // number_of
    chance = jax.random.randint(jax.random.fold_in(key, 2), (rows, number_of), 0, 4096) + favour
    holders = jax.random.permutation(jax.random.fold_in(key, 3), rows)[jnp.arange(number_of) % rows]
    chance = jnp.where(jnp.arange(rows)[:, None] == holders[None, :], 1 << 14, chance)
    priority = chance * number_of + jnp.arange(number_of)
    return lax.top_k(priority.astype(jnp.int32), top)[1].astype(jnp.int32)


def scatter_about(own_key, dims, scale, bound, split=(), held_as=jnp.bfloat16):
    result = scale * jax.random.normal(own_key, dims, jnp.float32)
    if split:
        result = result * levels(own_key, dims, split, -0.22, 0.18)
    return jnp.clip(result, -bound, bound).astype(held_as)


def setup_inputs(seed: int = 0) -> dict:
    splits = jax.random.split(jax.random.key(seed), 8)
    return {
        "tokens": scatter_about(splits[0], (CLIPS, FRAMES, PATCHES, D), 1.0, 6.0, ((0, 8), (1, 4))),
        "gain": jnp.clip(1.0 + 0.15 * jax.random.normal(splits[1], (D,), jnp.float32), 0.25, 1.75).astype(jnp.bfloat16),
        "w_qkv": scatter_about(splits[2], (D, 3 * D), D ** -0.5, 0.1875, ((0, 8),)),
        "w_out": scatter_about(splits[3], (D, D), D ** -0.5, 0.1875, ((0, 8),)),
        "w_pair": scatter_about(splits[4], (2, D, LATENT), (D // PATCHES) ** -0.5, 3.0, (), jnp.float32),
        "codebook": scatter_about(splits[5], (CODES, LATENT), 1.0, 5.0, (), jnp.float32),
        "codes": distinct(splits[6], CLIPS * FRAMES, CODES, 1, 1024).reshape((CLIPS, FRAMES, 1)),
    }


EPS = 1e-06
BETA = 0.25

def normalize(xf, gain):
    scale = lax.rsqrt(lax.optimization_barrier(jnp.mean(xf * xf, axis=-1, keepdims=True)) + EPS)
    return (xf * scale * gain.astype(jnp.float32)).astype(jnp.bfloat16)

def project(normed, weight):
    shape = normed.shape
    flat = jnp.dot(normed.reshape(-1, shape[-1]), weight, preferred_element_type=jnp.float32)
    return flat.astype(jnp.bfloat16).reshape(shape[:-1] + (3, shape[-1]))

def attend(qkv):
    clips, frames, patches, _, width = qkv.shape
    local_heads = width // HEAD_DIM
    parts = qkv.reshape(clips, frames, patches, 3, local_heads, HEAD_DIM)
    query = parts[:, :, :, 0].astype(jnp.float32)
    keys = parts[:, :, :, 1].astype(jnp.float32)
    values = parts[:, :, :, 2].astype(jnp.float32)
    scores = jnp.einsum('cfphd,cgphd->cphfg', query, keys) * HEAD_DIM ** (-0.5)
    causal = jnp.arange(frames)[:, None] >= jnp.arange(frames)[None, :]
    scores = jnp.where(causal, scores, -1e+30)
    weights = jax.nn.softmax(scores, axis=-1).astype(jnp.bfloat16)
    mixed = jnp.einsum('cphfg,cgphd->cfphd', weights.astype(jnp.float32), values)
    return mixed.reshape(clips, frames, patches, width).astype(jnp.bfloat16)

def output(xf, attended, weight):
    shape = xf.shape
    moved = jnp.dot(attended.reshape(-1, shape[-1]), weight, preferred_element_type=jnp.float32)
    return lax.optimization_barrier(jnp.mean(xf + moved.reshape(shape), axis=2))

def reference(tokens, gain, w_qkv, w_out, w_pair, codebook, codes):

    def whole(xf):
        return output(xf, attend(project(normalize(xf, gain), w_qkv)), w_out)

    def forward(clip):
        return whole(clip[None].astype(jnp.float32))[0]
    pooled = lax.map(forward, tokens)
    following = jnp.concatenate([pooled[:, 1:], jnp.zeros_like(pooled[:, :1])], axis=1)
    flat_now = pooled.reshape(-1, D)
    flat_next = following.reshape(-1, D)
    hp = lax.Precision.HIGHEST
    action = jnp.dot(flat_now, w_pair[0], precision=hp) + jnp.dot(flat_next, w_pair[1], precision=hp)
    onehot = (codes.reshape(-1)[:, None] == jnp.arange(CODES)[None, :]).astype(jnp.float32)
    quantized = jnp.dot(onehot, codebook, precision=hp)
    diff = action - quantized
    d_action = 2.0 * BETA * diff
    d_quant = -2.0 * diff
    count = lax.optimization_barrier(jnp.sum(onehot, axis=0))
    codebook_step = jnp.dot(onehot.T, d_quant, precision=hp) / count[:, None]
    grad_pair = jnp.stack([jnp.dot(flat_now.T, d_action, precision=hp), jnp.dot(flat_next.T, d_action, precision=hp)])
    d_own = jnp.dot(d_action, w_pair[0].T, precision=hp).reshape(pooled.shape)
    d_next = jnp.dot(d_action, w_pair[1].T, precision=hp).reshape(pooled.shape)
    carried = jnp.concatenate([jnp.zeros_like(d_next[:, :1]), d_next[:, :-1]], axis=1)
    d_pooled = (d_own + carried) * PATCHES

    def backward(pair):
        clip, cotangent = pair
        _, pull = jax.vjp(whole, clip[None].astype(jnp.float32))
        return pull(cotangent[None])[0][0].astype(jnp.bfloat16)
    grad_tokens = lax.map(backward, (tokens, d_pooled))
    return (grad_tokens, grad_pair, codebook_step)
```

```python
import functools

import jax
import jax.numpy as jnp
from jax import lax
from jax.experimental import pallas as pl
from jax.experimental.pallas import tpu as pltpu
from jax.sharding import PartitionSpec as P

HEAD_DIM = 64
EPS = 1e-06
BETA = 0.25
LANES = 128
F32 = jnp.float32
BF16 = jnp.bfloat16
HIGH = lax.Precision.HIGHEST


def dot(a, b, ca=1, cb=0, precision=None):
    return lax.dot_general(
        a, b, (((ca,), (cb,)), ((), ())), precision=precision, preferred_element_type=F32
    )


def dot_split(a, b, cb=0):
    high = a.astype(BF16)
    rest = a - high.astype(F32)
    mid = rest.astype(BF16)
    low = (rest - mid.astype(F32)).astype(BF16)
    n = a.shape[0]
    terms = jnp.concatenate([high.astype(F32), mid.astype(F32), low.astype(F32)], axis=0)
    out = dot(terms.astype(BF16), b, 1, cb)
    return out[:n] + out[n : 2 * n] + out[2 * n :]


def bits_of(n):
    return max(n.bit_length() - 1, 0)


def ring_place(chip, n):
    b = [(chip // 2**k) % 2 for k in range(bits_of(n))]
    return sum(((sum(b[k:]) % 2) * 2**k for k in range(len(b))), 0)


def ring_chip(place, n):
    count = bits_of(n)
    b = [(place // 2**k) % 2 for k in range(count)] + [0]
    return sum((((b[k] + b[k + 1]) % 2) * 2**k for k in range(count)), 0)


def kernel(
    cfg, tokens, gain, wq_own, wo_own, w_pair, codebook, codes,
    out, pair_out, step_out,
    wq, wo, x, normed, acc, qkv, bias, probs, attended, sums, sums_all, pack, pack_all,
    d_rows, d_att, dqkv, dn_send, dn_recv, send, recv, local_sem,
):
    dp, tm, rows, patches, width, latent, n_codes = cfg
    mine = patches // tm
    total = tm * mine
    fp = sums.shape[1]
    chips = dp // 2
    half_ring = chips // 2
    i = lax.axis_index("dp")
    t = lax.axis_index("tm")
    core = i % 2
    place = ring_place(i // 2, chips)

    def device_at(p, c):
        return ring_chip((p + 2 * chips) % chips, chips) * 2 + c

    barrier = pltpu.get_barrier_semaphore()
    for r in range(1, tm):
        pl.semaphore_signal(barrier, inc=1, device_id={"dp": i, "tm": (t + r) % tm})
    for r in range(1, dp):
        pl.semaphore_signal(barrier, inc=1, device_id={"dp": (i + r) % dp, "tm": t})
    pl.semaphore_wait(barrier, tm + dp - 2)

    tags = {}

    def tag(*key):
        return tags.setdefault(key, len(tags))

    started = []

    def remote(src, dst, key, dpi, tmi):
        k = tag(*key)
        return pltpu.make_async_remote_copy(
            src_ref=src, dst_ref=dst, send_sem=send.at[k], recv_sem=recv.at[k],
            device_id={"dp": dpi, "tm": tmi},
        )

    def go(copy):
        copy.start()
        started.append(copy)

    mats = (wq, wo)
    owns = (wq_own, wo_own)
    half = rows // 2
    dirs = (1, -1)

    def piece(m, origin, h):
        return mats[m].at[pl.ds(pl.multiple_of(origin * rows + h * half, half), half)]

    def own_piece(m, h):
        return owns[m].at[pl.ds(h * half, half)]

    def main_half(d):
        return 0 if dirs[d] == 1 else 1

    def halves(d, s):
        first = main_half(d)
        return (first, 1 - first) if s < half_ring - 1 else (first,)

    def ring_copy(m, d, s, h):
        origin = device_at(place - dirs[d] * s, core)
        src = own_piece(m, h) if s == 0 else piece(m, origin, h)
        return remote(src, piece(m, origin, h), ("ring", m, d, s, h), device_at(place + dirs[d], core), t)

    def sib_copy(m, d, s, h):
        origin = device_at(place - dirs[d] * s, core)
        src = own_piece(m, h) if s == 0 else piece(m, origin, h)
        return remote(src, piece(m, origin, h), ("sib", m, d, s, h), device_at(place, 1 - core), t)

    def start_own(m):
        for n in range(2):
            for d in range(2):
                if n < len(halves(d, 0)):
                    go(ring_copy(m, d, 0, halves(d, 0)[n]))
        for h in range(2):
            go(sib_copy(m, 0, 0, h))

    def take(m, d, s, h):
        ring_copy(m, d, s, h).wait_recv()
        if s + 1 < half_ring and h in halves(d, s + 1):
            go(ring_copy(m, d, s + 1, h))
        go(sib_copy(m, d, s + 1, h))

    for r in sorted(range(1, tm), key=lambda r: -min(r, tm - r)):
        other = (t + r) % tm
        go(remote(
            tokens.at[pl.ds(pl.multiple_of(other * mine, mine), mine)],
            x.at[pl.ds(pl.multiple_of(t * mine, mine), mine)], ("tok", r), i, other,
        ))
    start_own(0)
    here = [
        pltpu.make_async_copy(wq_own, wq.at[pl.ds(pl.multiple_of(i * rows, rows), rows)], local_sem.at[0]),
        pltpu.make_async_copy(wo_own, wo.at[pl.ds(pl.multiple_of(i * rows, rows), rows)], local_sem.at[1]),
        pltpu.make_async_copy(
            tokens.at[pl.ds(pl.multiple_of(t * mine, mine), mine)],
            x.at[pl.ds(pl.multiple_of(t * mine, mine), mine)], local_sem.at[2],
        ),
    ]
    for copy in here:
        copy.start()

    row = lax.broadcasted_iota(jnp.int32, (total, total), 0)
    col = lax.broadcasted_iota(jnp.int32, (total, total), 1)
    seen = (row % mine == col % mine) & (row // mine >= col // mine)
    bias[...] = jnp.where(seen, 0.0, -1e30).astype(F32)

    def first_main(m):
        for s in range(half_ring):
            for d in range(2):
                take(m, d, s, main_half(d))

    def rest_of(m):
        for s in range(half_ring):
            for d in range(2):
                for h in halves(d, s)[1:]:
                    take(m, d, s, h)

    if half_ring > 1:
        for d in range(2):
            take(0, d, 0, main_half(d))
    start_own(1)

    for copy in here:
        copy.wait()
    for r in range(1, tm):
        remote(
            tokens.at[pl.ds(0, mine)], x.at[pl.ds(pl.multiple_of(t * mine, mine), mine)], ("tok", r), i, t
        ).wait_recv()

    block = 32

    def norm_step(b, carry):
        at = pl.ds(pl.multiple_of(b * block, block), block)
        xf = x[at, :].astype(F32)
        scale = lax.rsqrt(jnp.mean(xf * xf, axis=-1, keepdims=True) + EPS)
        normed[at, :] = (xf * scale * gain[...].astype(F32)).astype(BF16)
        return carry

    lax.fori_loop(0, total // block, norm_step, 0)

    pair = 2 * rows
    columns = 512

    def project(p, first, last):
        base = pl.multiple_of(ring_chip((p + 2 * chips) % chips, chips) * pair, pair)

        def body(n, carry):
            at = pl.ds(pl.multiple_of(n * columns, columns), columns)
            part = dot(normed[:, pl.ds(base, pair)], wq[pl.ds(base, pair), at])
            if not first:
                part = part + acc[:, at]
            if last:
                qkv[:, at] = part.astype(BF16)
            else:
                acc[:, at] = part
            return carry

        lax.fori_loop(0, 3 * width // columns, body, 0)

    def wait_sib(m, d, s, h):
        sib_copy(m, d, s, h).wait_recv()

    by_chip = pair % LANES == 0
    for h in range(2):
        wait_sib(0, 0, 0, h)
    if by_chip:
        project(place, True, chips == 1)
    for s in range(half_ring):
        for d in range(2):
            for n, h in enumerate(halves(d, s)):
                if not (half_ring > 1 and s == 0 and n == 0):
                    take(0, d, s, h)
        for d in range(2):
            for h in halves(d, s):
                wait_sib(0, d, s + 1, h)
            if by_chip and s < half_ring - 1:
                project(place - dirs[d] * (s + 1), False, False)
    if by_chip:
        project(place + half_ring, False, True)
    else:
        def whole_body(n, carry):
            at = pl.ds(pl.multiple_of(n * columns, columns), columns)
            qkv[:, at] = dot(normed[...], wq[:, at]).astype(BF16)
            return carry

        lax.fori_loop(0, 3 * width // columns, whole_body, 0)

    per = LANES // HEAD_DIM
    lane = lax.broadcasted_iota(jnp.int32, (total, LANES), 1)
    scale_q = HEAD_DIM ** (-0.5)

    def only(value, j):
        return jnp.where(lane // HEAD_DIM == j, value, jnp.zeros_like(value))

    def lanes_at(b, part):
        return pl.ds(pl.multiple_of(part * width + b * LANES, LANES), LANES)

    def forward(b, carry):
        q, k, v = (qkv[:, lanes_at(b, n)] for n in range(3))
        mixed = None
        for j in range(per):
            scores = dot(only(q, j), k, 1, 1) * scale_q + bias[...]
            e = jnp.exp(scores - jnp.max(scores, axis=-1, keepdims=True))
            w = e / jnp.sum(e, axis=-1, keepdims=True)
            probs[b * per + j] = w
            term = dot(w.astype(BF16), only(v, j))
            mixed = term if mixed is None else mixed + term
        attended[:, lanes_at(b, 0)] = mixed.astype(BF16)
        return carry

    lax.fori_loop(0, width // LANES, forward, 0)

    frow = lax.broadcasted_iota(jnp.int32, (fp, total), 0)
    fcol = lax.broadcasted_iota(jnp.int32, (fp, total), 1)
    member = jnp.where(fcol // mine == frow, 1.0, 0.0).astype(BF16)
    sums[0] = dot(member, attended[...])
    sums[1] = dot(member, x[...])
    r8 = lax.broadcasted_iota(jnp.int32, (fp, width), 0)
    l8 = lax.broadcasted_iota(jnp.int32, (fp, width), 1)
    sums[2] = jnp.where((r8 == t) & (l8 == codes[0, 0]), 1.0, 0.0).astype(F32)
    for r in range(1, tm):
        go(remote(sums, sums_all.at[t], ("sum", r), i, (t + r) % tm))

    for s in range(half_ring):
        for d in range(2):
            for h in halves(d, s):
                take(1, d, s, h)
    sums_all[t] = sums[...]
    for h in range(2):
        wait_sib(1, 0, 0, h)
    for s in range(half_ring):
        for d in range(2):
            for h in halves(d, s):
                wait_sib(1, d, s + 1, h)
    for r in range(1, tm):
        remote(sums, sums_all.at[t], ("sum", r), i, t).wait_recv()

    tot = sums_all[0]
    for r in range(1, tm):
        tot = tot + sums_all[r]
    onehot = tot[2][:, :LANES]
    pooled = tot[1] * (1.0 / patches) + dot_split(tot[0] * (1.0 / patches), wo[...])
    rfull = lax.broadcasted_iota(jnp.int32, (fp, width), 0)
    following = jnp.where(rfull < tm - 1, pltpu.roll(pooled, fp - 1, 0), 0.0)
    action = dot(pooled, w_pair[0], precision=HIGH) + dot(following, w_pair[1], precision=HIGH)
    quantized = dot(onehot[:, :n_codes], codebook[...], precision=HIGH)
    diff = action - quantized
    d_action = (2.0 * BETA) * diff
    pack[0] = pooled
    pack[1] = following
    pack[2] = jnp.zeros((fp, width), F32)
    pack[2, :, 0:latent] = diff
    pack[2, :, LANES : 2 * LANES] = onehot
    d_own = dot(d_action, w_pair[0], 1, 1, precision=HIGH)
    d_next = dot(d_action, w_pair[1], 1, 1, precision=HIGH)
    carried = jnp.where((rfull > 0) & (rfull < tm), pltpu.roll(d_next, 1, 0), 0.0)
    d_pooled = d_own + carried
    d_rows[...] = d_pooled
    d_att[...] = dot_split(d_pooled, wo[...], 1).astype(BF16)
    for r in range(1, dp):
        go(remote(pack, pack_all.at[i], ("pack", r), (i + r) % dp, t))

    mrow = lax.broadcasted_iota(jnp.int32, (total, fp), 0)
    mcol = lax.broadcasted_iota(jnp.int32, (total, fp), 1)
    spread = jnp.where(mrow // mine == mcol, 1.0, 0.0).astype(BF16)

    def backward(b, carry):
        q, k, v = (qkv[:, lanes_at(b, n)] for n in range(3))
        d_out = dot(spread, d_att[:, lanes_at(b, 0)]).astype(BF16)
        dq = dk = dv = jnp.zeros((total, LANES), F32)
        for j in range(per):
            w = probs[b * per + j]
            d_w = dot(only(d_out, j), v, 1, 1).astype(BF16).astype(F32)
            wd = w * d_w
            d_s = ((wd - w * jnp.sum(wd, axis=-1, keepdims=True)) * scale_q).astype(BF16)
            dq = dq + dot(d_s, only(k, j))
            dk = dk + dot(d_s, only(q, j), 0, 0)
            dv = dv + dot(w.astype(BF16), only(d_out, j), 0, 0)
        dqkv[:, lanes_at(b, 0)] = dq.astype(BF16)
        dqkv[:, lanes_at(b, 1)] = dk.astype(BF16)
        dqkv[:, lanes_at(b, 2)] = dv.astype(BF16)
        return carry

    lax.fori_loop(0, width // LANES, backward, 0)

    pieces = dn_send.shape[0]
    wide = width // pieces
    for c in range(pieces):
        dn_send[c] = dot(dqkv[...], wq[c * wide : (c + 1) * wide, :], 1, 1).astype(BF16)
        for r in sorted(range(1, tm), key=lambda r: -min(r, tm - r)):
            other = (t + r) % tm
            go(remote(
                dn_send.at[c, pl.ds(pl.multiple_of(other * mine, mine), mine)],
                dn_recv.at[c, pl.ds(pl.multiple_of(t * mine, mine), mine)], ("dn", c, r), i, other,
            ))
        at = pl.ds(pl.multiple_of(t * mine, mine), mine)
        dn_recv[c, at, :] = dn_send[c, at, :]

    pack_all[i] = pack[...]
    for r in range(1, dp):
        remote(pack, pack_all.at[i], ("pack", r), i, t).wait_recv()
    every = dp * fp
    now_all = pack_all[:, 0].reshape(every, width)
    next_all = pack_all[:, 1].reshape(every, width)
    diff_all = pack_all[:, 2, :, :LANES].reshape(every, LANES)
    hot_all = pack_all[:, 2, :, LANES : 2 * LANES].reshape(every, LANES)
    da_all = (2.0 * BETA) * diff_all
    pair_out[0] = dot(da_all, now_all, 0, 0, precision=HIGH)[:latent]
    pair_out[1] = dot(da_all, next_all, 0, 0, precision=HIGH)[:latent]
    code_total = dot(hot_all, -2.0 * diff_all, 0, 0, precision=HIGH)
    count = dot(hot_all, jnp.ones((every, LANES), F32), 0, 0, precision=HIGH)
    step_out[...] = code_total[:n_codes, :latent] / count[:n_codes, :latent]

    for c in range(pieces):
        for r in range(1, tm):
            remote(
                dn_send.at[c, pl.ds(0, mine)],
                dn_recv.at[c, pl.ds(pl.multiple_of(t * mine, mine), mine)], ("dn", c, r), i, t,
            ).wait_recv()
    d_resid = d_rows[pl.ds(t, 1), :]

    def finish(b, carry):
        at = pl.ds(pl.multiple_of(b * block, block), block)
        xf = tokens[at, :].astype(F32)
        scale = lax.rsqrt(jnp.mean(xf * xf, axis=-1, keepdims=True) + EPS)
        dn = jnp.concatenate([dn_recv[c, at, :] for c in range(pieces)], axis=1).astype(F32)
        u = dn * gain[...].astype(F32)
        inner = jnp.mean(xf * u, axis=-1, keepdims=True)
        dx = u * scale - xf * (scale * scale * scale * inner)
        out[at, :] = (d_resid + dx).astype(BF16)
        return carry

    lax.fori_loop(0, total // block, finish, 0)
    for copy in started:
        copy.wait_send()
    assert len(tags) <= send.shape[0]


def local(dp, tm, tokens, gain, w_qkv, w_out, w_pair, codebook, codes):
    patches, width = tokens.shape[2:]
    rows = w_qkv.shape[0]
    latent, n_codes = w_pair.shape[2], codebook.shape[0]
    fp = -(-tm // 8) * 8
    heads = width // HEAD_DIM
    pieces = 4
    tags = (tm - 1) * (2 + pieces) + (dp - 1) + 8 * dp + 16
    vmem = pl.BlockSpec(memory_space=pltpu.VMEM)
    grad, pair, step = pl.pallas_call(
        functools.partial(kernel, (dp, tm, rows, patches, width, latent, n_codes)),
        out_shape=(
            jax.ShapeDtypeStruct((patches, width), BF16),
            jax.ShapeDtypeStruct((2, latent, width), F32),
            jax.ShapeDtypeStruct((n_codes, latent), F32),
        ),
        in_specs=[vmem] * 6 + [pl.BlockSpec(memory_space=pltpu.SMEM)],
        out_specs=(vmem, vmem, vmem),
        scratch_shapes=[
            pltpu.VMEM((dp * rows, 3 * width), BF16),
            pltpu.VMEM((dp * rows, width), BF16),
            pltpu.VMEM((patches, width), BF16),
            pltpu.VMEM((patches, width), BF16),
            pltpu.VMEM((patches, 3 * width), F32),
            pltpu.VMEM((patches, 3 * width), BF16),
            pltpu.VMEM((patches, patches), F32),
            pltpu.VMEM((heads, patches, patches), F32),
            pltpu.VMEM((patches, width), BF16),
            pltpu.VMEM((3, fp, width), F32),
            pltpu.VMEM((tm, 3, fp, width), F32),
            pltpu.VMEM((3, fp, width), F32),
            pltpu.VMEM((dp, 3, fp, width), F32),
            pltpu.VMEM((fp, width), F32),
            pltpu.VMEM((fp, width), BF16),
            pltpu.VMEM((patches, 3 * width), BF16),
            pltpu.VMEM((pieces, patches, width // pieces), BF16),
            pltpu.VMEM((pieces, patches, width // pieces), BF16),
            pltpu.SemaphoreType.DMA((tags,)),
            pltpu.SemaphoreType.DMA((tags,)),
            pltpu.SemaphoreType.DMA((3,)),
        ],
        compiler_params=pltpu.CompilerParams(
            collective_id=0, has_side_effects=True, vmem_limit_bytes=60 * 1024 * 1024
        ),
    )(
        tokens.reshape(patches, width), gain.reshape(1, width), w_qkv, w_out, w_pair, codebook,
        codes.reshape(1, 1),
    )
    return grad.reshape(tokens.shape), pair.swapaxes(1, 2), step


def solution(mesh):
    placed = (
        P("dp", "tm", None, None),
        P(),
        P("dp", None),
        P("dp", None),
        P(),
        P(),
        P("dp", "tm", None),
    )
    return jax.shard_map(
        functools.partial(local, mesh.shape["dp"], mesh.shape["tm"]),
        mesh=mesh,
        in_specs=placed,
        out_specs=(P("dp", "tm", None, None), P(), P()),
        check_vma=False,
    )
```

```python
import functools

import jax
import jax.numpy as jnp
from jax import lax
from jax.experimental import pallas as pl
from jax.experimental.pallas import tpu as pltpu
from jax.sharding import PartitionSpec as P

HEAD_DIM = 64
EPS = 1e-06
BETA = 0.25
LANES = 128
F32 = jnp.float32
BF16 = jnp.bfloat16
HIGH = lax.Precision.HIGHEST


def dot(a, b, ca=1, cb=0, precision=None):
    return lax.dot_general(
        a, b, (((ca,), (cb,)), ((), ())), precision=precision, preferred_element_type=F32
    )


def dot_split(a, b, cb=0):
    high = a.astype(BF16)
    rest = a - high.astype(F32)
    mid = rest.astype(BF16)
    low = (rest - mid.astype(F32)).astype(BF16)
    n = a.shape[0]
    terms = jnp.concatenate([high.astype(F32), mid.astype(F32), low.astype(F32)], axis=0)
    out = dot(terms.astype(BF16), b, 1, cb)
    return out[:n] + out[n : 2 * n] + out[2 * n :]


def bits_of(n):
    return max(n.bit_length() - 1, 0)


def ring_place(chip, n):
    b = [(chip // 2**k) % 2 for k in range(bits_of(n))]
    return sum(((sum(b[k:]) % 2) * 2**k for k in range(len(b))), 0)


def ring_chip(place, n):
    count = bits_of(n)
    b = [(place // 2**k) % 2 for k in range(count)] + [0]
    return sum((((b[k] + b[k + 1]) % 2) * 2**k for k in range(count)), 0)


def kernel(
    cfg, tokens, gain, wq_own, wo_own, w_pair, codebook, codes,
    out, pair_out, step_out,
    wq, wo, x, normed, acc, qkv, bias, probs, attended, sums, sums_all, pack, pack_all,
    d_rows, d_att, dqkv, dn_send, dn_recv, send, recv, local_sem,
):
    dp, tm, rows, patches, width, latent, n_codes, groups = cfg
    mine = patches // tm
    total = tm * mine
    sub = mine // groups
    part_rows = tm * sub
    fp = sums.shape[1]
    chips = dp // 2
    half_ring = chips // 2
    i = lax.axis_index("dp")
    t = lax.axis_index("tm")
    core = i % 2
    place = ring_place(i // 2, chips)

    def device_at(p, c):
        return ring_chip((p + 2 * chips) % chips, chips) * 2 + c

    barrier = pltpu.get_barrier_semaphore()
    for r in range(1, tm):
        pl.semaphore_signal(barrier, inc=1, device_id={"dp": i, "tm": (t + r) % tm})
    for r in range(1, dp):
        pl.semaphore_signal(barrier, inc=1, device_id={"dp": (i + r) % dp, "tm": t})
    pl.semaphore_wait(barrier, tm + dp - 2)

    tags = {}

    def tag(*key):
        return tags.setdefault(key, len(tags))

    started = []

    def remote(src, dst, key, dpi, tmi):
        k = tag(*key)
        return pltpu.make_async_remote_copy(
            src_ref=src, dst_ref=dst, send_sem=send.at[k], recv_sem=recv.at[k],
            device_id={"dp": dpi, "tm": tmi},
        )

    def go(copy):
        copy.start()
        started.append(copy)

    mats = (wq, wo)
    owns = (wq_own, wo_own)
    half = rows // 2
    dirs = (1, -1)

    quarter = half // 2
    sharing = half_ring == 2 and quarter % 16 == 0 and tm % 2 == 0
    odd = t % 2
    twin = t + 1 - 2 * odd

    def piece(m, origin, h):
        return mats[m].at[pl.ds(pl.multiple_of(origin * rows + h * half, half), half)]

    def own_piece(m, h):
        return owns[m].at[pl.ds(h * half, half)]

    def split(m, d, s, h):
        return sharing and m == 0 and s == 0 and h != main_half(d)

    def quarter_of(m, origin, h, which):
        at = origin * rows + h * half + which * quarter
        return mats[m].at[pl.ds(pl.multiple_of(at, quarter), quarter)]

    def own_quarter(m, h, which):
        return owns[m].at[pl.ds(pl.multiple_of(h * half + which * quarter, quarter), quarter)]

    def main_half(d):
        return 0 if dirs[d] == 1 else 1

    def halves(d, s):
        first = main_half(d)
        return (first, 1 - first) if s < half_ring - 1 else (first,)

    def ring_copy(m, d, s, h):
        origin = device_at(place - dirs[d] * s, core)
        if split(m, d, s, h):
            return remote(
                own_quarter(m, h, odd), quarter_of(m, origin, h, odd), ("ring", m, d, s, h),
                device_at(place + dirs[d], core), t,
            )
        src = own_piece(m, h) if s == 0 else piece(m, origin, h)
        return remote(src, piece(m, origin, h), ("ring", m, d, s, h), device_at(place + dirs[d], core), t)

    def sib_copy(m, d, s, h):
        origin = device_at(place - dirs[d] * s, core)
        src = own_piece(m, h) if s == 0 else piece(m, origin, h)
        return remote(src, piece(m, origin, h), ("sib", m, d, s, h), device_at(place, 1 - core), t)

    def twin_copy(d):
        h = 1 - main_half(d)
        at = quarter_of(0, device_at(place - dirs[d], core), h, odd)
        return remote(at, at, ("twin", d), i, twin)

    def quarter_sib(d, n):
        h = 1 - main_half(d)
        which = odd if n == 0 else 1 - odd
        at = quarter_of(0, device_at(place - dirs[d], core), h, which)
        return remote(at, at, ("quarter", d, n), device_at(place, 1 - core), t)

    def start_own(m):
        for n in range(2):
            for d in range(2):
                if n < len(halves(d, 0)):
                    go(ring_copy(m, d, 0, halves(d, 0)[n]))
        for h in range(2):
            go(sib_copy(m, 0, 0, h))

    def take(m, d, s, h):
        ring_copy(m, d, s, h).wait_recv()
        if split(m, d, s, h):
            go(twin_copy(d))
            go(quarter_sib(d, 0))
            return
        if s + 1 < half_ring and h in halves(d, s + 1):
            go(ring_copy(m, d, s + 1, h))
        go(sib_copy(m, d, s + 1, h))

    for r in sorted(range(1, tm), key=lambda r: -min(r, tm - r)):
        other = (t + r) % tm
        for g in range(groups):
            go(remote(
                tokens.at[pl.ds(pl.multiple_of(other * mine + g * sub, sub), sub)],
                x.at[pl.ds(pl.multiple_of(g * part_rows + t * sub, sub), sub)], ("tok", r, g), i, other,
            ))
    start_own(0)
    here = [
        pltpu.make_async_copy(wq_own, wq.at[pl.ds(pl.multiple_of(i * rows, rows), rows)], local_sem.at[0]),
        pltpu.make_async_copy(wo_own, wo.at[pl.ds(pl.multiple_of(i * rows, rows), rows)], local_sem.at[1]),
    ] + [
        pltpu.make_async_copy(
            tokens.at[pl.ds(pl.multiple_of(t * mine + g * sub, sub), sub)],
            x.at[pl.ds(pl.multiple_of(g * part_rows + t * sub, sub), sub)], local_sem.at[2 + g],
        )
        for g in range(groups)
    ]
    for copy in here:
        copy.start()

    row = lax.broadcasted_iota(jnp.int32, (part_rows, part_rows), 0)
    col = lax.broadcasted_iota(jnp.int32, (part_rows, part_rows), 1)
    seen = (row % sub == col % sub) & (row // sub >= col // sub)
    bias[...] = jnp.where(seen, 0.0, -1e30).astype(F32)

    if half_ring > 1:
        for d in range(2):
            take(0, d, 0, main_half(d))
    start_own(1)

    for copy in here:
        copy.wait()
    for r in range(1, tm):
        for g in range(groups):
            remote(
                tokens.at[pl.ds(0, sub)], x.at[pl.ds(pl.multiple_of(g * part_rows + t * sub, sub), sub)],
                ("tok", r, g), i, t,
            ).wait_recv()

    block = 32

    def norm_step(b, carry):
        at = pl.ds(pl.multiple_of(b * block, block), block)
        xf = x[at, :].astype(F32)
        scale = lax.rsqrt(jnp.mean(xf * xf, axis=-1, keepdims=True) + EPS)
        normed[at, :] = (xf * scale * gain[...].astype(F32)).astype(BF16)
        return carry

    lax.fori_loop(0, total // block, norm_step, 0)

    frow = lax.broadcasted_iota(jnp.int32, (fp, total), 0)
    fcol = lax.broadcasted_iota(jnp.int32, (fp, total), 1)
    member = jnp.where((fcol % part_rows) // sub == frow, 1.0, 0.0).astype(BF16)
    sums[1] = dot(member, x[...])
    r8 = lax.broadcasted_iota(jnp.int32, (fp, width), 0)
    l8 = lax.broadcasted_iota(jnp.int32, (fp, width), 1)
    sums[2] = jnp.where((r8 == t) & (l8 == codes[0, 0]), 1.0, 0.0).astype(F32)

    pair = 2 * rows
    columns = 512

    def project(p, first, last):
        base = pl.multiple_of(ring_chip((p + 2 * chips) % chips, chips) * pair, pair)

        def body(n, carry):
            at = pl.ds(pl.multiple_of(n * columns, columns), columns)
            part = dot(normed[:, pl.ds(base, pair)], wq[pl.ds(base, pair), at])
            if not first:
                part = part + acc[:, at]
            if last:
                qkv[:, at] = part.astype(BF16)
            else:
                acc[:, at] = part
            return carry

        lax.fori_loop(0, 3 * width // columns, body, 0)

    def wait_sib(m, d, s, h):
        sib_copy(m, d, s, h).wait_recv()

    by_chip = pair % LANES == 0
    for h in range(2):
        wait_sib(0, 0, 0, h)
    if by_chip:
        project(place, True, chips == 1)
    if sharing:
        for d in range(2):
            take(0, d, 0, 1 - main_half(d))
        for d in range(2):
            twin_copy(d).wait_recv()
            go(quarter_sib(d, 1))
        for d in range(2):
            wait_sib(0, d, 1, main_half(d))
            for n in range(2):
                quarter_sib(d, n).wait_recv()
            if by_chip:
                project(place - dirs[d], False, False)
            if d == 0:
                for e in range(2):
                    take(0, e, 1, main_half(e))
        for d in range(2):
            wait_sib(0, d, 2, main_half(d))
    else:
        for s in range(half_ring):
            for d in range(2):
                for n, h in enumerate(halves(d, s)):
                    if not (half_ring > 1 and s == 0 and n == 0):
                        take(0, d, s, h)
            for d in range(2):
                for h in halves(d, s):
                    wait_sib(0, d, s + 1, h)
                if by_chip and s < half_ring - 1:
                    project(place - dirs[d] * (s + 1), False, False)
    for r in range(1, tm):
        go(remote(sums.at[pl.ds(1, 2)], sums_all.at[t, pl.ds(1, 2)], ("early", r), i, (t + r) % tm))
    if by_chip:
        project(place + half_ring, False, True)
    else:
        def whole_body(n, carry):
            at = pl.ds(pl.multiple_of(n * columns, columns), columns)
            qkv[:, at] = dot(normed[...], wq[:, at]).astype(BF16)
            return carry

        lax.fori_loop(0, 3 * width // columns, whole_body, 0)

    if half_ring > 1:
        for d in range(2):
            take(1, d, 0, main_half(d))

    per = LANES // HEAD_DIM
    lane = lax.broadcasted_iota(jnp.int32, (part_rows, LANES), 1)
    scale_q = HEAD_DIM ** (-0.5)

    def only(value, j):
        return jnp.where(lane // HEAD_DIM == j, value, jnp.zeros_like(value))

    def lanes_at(b, part):
        return pl.ds(part * width + b * LANES, LANES)

    heads = width // HEAD_DIM

    def group(g):
        return pl.ds(g * part_rows, part_rows)

    def forward(b):
        chains = [(g, j) for g in range(groups) for j in range(per)]
        q, k, v = ([qkv[group(g), lanes_at(b, n)] for g in range(groups)] for n in range(3))
        scores = [dot(only(q[g], j), k[g], 1, 1) * scale_q + bias[...] for g, j in chains]
        tops = [jnp.max(value, axis=-1, keepdims=True) for value in scores]
        raised = [jnp.exp(value - top) for value, top in zip(scores, tops)]
        totals = [jnp.sum(value, axis=-1, keepdims=True) for value in raised]
        ws = [value / whole for value, whole in zip(raised, totals)]
        for (g, j), w in zip(chains, ws):
            probs[g * heads + b * per + j] = w
        terms = [dot(w.astype(BF16), only(v[g], j)) for (g, j), w in zip(chains, ws)]
        for g in range(groups):
            attended[group(g), lanes_at(b, 0)] = sum(terms[g * per + 1 : g * per + per], terms[g * per]).astype(BF16)

    blocks = width // LANES
    for b in range(blocks):
        forward(b)

    sums[0] = dot(member, attended[...])
    for r in range(1, tm):
        go(remote(sums.at[0], sums_all.at[t, 0], ("sum", r), i, (t + r) % tm))

    for s in range(half_ring):
        for d in range(2):
            for n, h in enumerate(halves(d, s)):
                if not (half_ring > 1 and s == 0 and n == 0):
                    take(1, d, s, h)
    sums_all[t] = sums[...]
    for h in range(2):
        wait_sib(1, 0, 0, h)
    for s in range(half_ring):
        for d in range(2):
            for h in halves(d, s):
                wait_sib(1, d, s + 1, h)
    for r in range(1, tm):
        remote(sums.at[0], sums_all.at[t, 0], ("sum", r), i, t).wait_recv()
        remote(sums.at[pl.ds(1, 2)], sums_all.at[t, pl.ds(1, 2)], ("early", r), i, t).wait_recv()

    tot = sums_all[0]
    for r in range(1, tm):
        tot = tot + sums_all[r]
    onehot = tot[2][:, :LANES]
    pooled = tot[1] * (1.0 / patches) + dot_split(tot[0] * (1.0 / patches), wo[...])
    rfull = lax.broadcasted_iota(jnp.int32, (fp, width), 0)
    following = jnp.where(rfull < tm - 1, pltpu.roll(pooled, fp - 1, 0), 0.0)
    action = dot(pooled, w_pair[0], 1, 1, HIGH) + dot(following, w_pair[1], 1, 1, HIGH)
    quantized = dot(onehot[:, :n_codes], codebook[...], precision=HIGH)
    diff = action - quantized
    d_action = (2.0 * BETA) * diff
    pack[0] = pooled
    pack[1] = following
    pack[2] = jnp.zeros((fp, width), F32)
    pack[2, :, 0:latent] = diff
    pack[2, :, LANES : 2 * LANES] = onehot
    d_own = dot(d_action, w_pair[0], precision=HIGH)
    d_next = dot(d_action, w_pair[1], precision=HIGH)
    carried = jnp.where((rfull > 0) & (rfull < tm), pltpu.roll(d_next, 1, 0), 0.0)
    d_pooled = d_own + carried
    d_rows[...] = d_pooled
    d_att[...] = dot_split(d_pooled, wo[...], 1).astype(BF16)
    for r in range(1, dp):
        go(remote(pack, pack_all.at[i], ("pack", r), (i + r) % dp, t))

    mrow = lax.broadcasted_iota(jnp.int32, (part_rows, fp), 0)
    mcol = lax.broadcasted_iota(jnp.int32, (part_rows, fp), 1)
    spread = jnp.where(mrow // sub == mcol, 1.0, 0.0).astype(BF16)

    def backward(g, near):
        chains = [(b, j) for b in near for j in range(per)]
        q, k, v = ({b: qkv[group(g), lanes_at(b, n)] for b in near} for n in range(3))
        d_out = {b: dot(spread, d_att[:, lanes_at(b, 0)]).astype(BF16) for b in near}
        ws = [probs[g * heads + b * per + j] for b, j in chains]
        d_ws = [dot(only(d_out[b], j), v[b], 1, 1).astype(BF16).astype(F32) for b, j in chains]
        wds = [w * d_w for w, d_w in zip(ws, d_ws)]
        means = [jnp.sum(wd, axis=-1, keepdims=True) for wd in wds]
        d_ss = [((wd - w * m) * scale_q).astype(BF16) for wd, w, m in zip(wds, ws, means)]
        dqs = [dot(d_s, only(k[b], j)) for (b, j), d_s in zip(chains, d_ss)]
        dks = [dot(d_s, only(q[b], j), 0, 0) for (b, j), d_s in zip(chains, d_ss)]
        dvs = [dot(w.astype(BF16), only(d_out[b], j), 0, 0) for (b, j), w in zip(chains, ws)]
        for n, b in enumerate(near):
            for part, terms in enumerate((dqs, dks, dvs)):
                mine_terms = terms[n * per : (n + 1) * per]
                dqkv[group(g), lanes_at(b, part)] = sum(mine_terms[1:], mine_terms[0]).astype(BF16)

    def dn_copy(c, g, r, other):
        return remote(
            dn_send.at[c, pl.ds(pl.multiple_of(g * part_rows + other * sub, sub), sub)],
            dn_recv.at[c, pl.ds(pl.multiple_of(t * mine + g * sub, sub), sub)], ("dn", c, g, r), i, other,
        )

    pieces = dn_send.shape[0]
    wide = width // pieces
    for g in range(groups):
        for b in range(0, blocks, 2):
            backward(g, tuple(range(b, min(b + 2, blocks))))
        for c in range(pieces):
            dn_send[c, group(g), :] = dot(dqkv[group(g), :], wq[c * wide : (c + 1) * wide, :], 1, 1).astype(BF16)
            for r in sorted(range(1, tm), key=lambda r: -min(r, tm - r)):
                go(dn_copy(c, g, r, (t + r) % tm))
            dn_recv[c, pl.ds(pl.multiple_of(t * mine + g * sub, sub), sub), :] = dn_send[
                c, pl.ds(pl.multiple_of(g * part_rows + t * sub, sub), sub), :
            ]

    pack_all[i] = pack[...]
    for r in range(1, dp):
        remote(pack, pack_all.at[i], ("pack", r), i, t).wait_recv()
    every = dp * fp
    now_all = pack_all[:, 0].reshape(every, width)
    next_all = pack_all[:, 1].reshape(every, width)
    diff_all = pack_all[:, 2, :, :LANES].reshape(every, LANES)
    hot_all = pack_all[:, 2, :, LANES : 2 * LANES].reshape(every, LANES)
    da_all = (2.0 * BETA) * diff_all
    pair_out[0] = dot(da_all, now_all, 0, 0, precision=HIGH)[:latent]
    pair_out[1] = dot(da_all, next_all, 0, 0, precision=HIGH)[:latent]
    code_total = dot(hot_all, -2.0 * diff_all, 0, 0, precision=HIGH)
    count = dot(hot_all, jnp.ones((every, LANES), F32), 0, 0, precision=HIGH)
    step_out[...] = code_total[:n_codes, :latent] / count[:n_codes, :latent]

    for g in range(groups):
        for c in range(pieces):
            for r in range(1, tm):
                dn_copy(c, g, r, t).wait_recv()
    d_resid = d_rows[pl.ds(t, 1), :]

    def finish(b, carry):
        at = pl.ds(pl.multiple_of(b * block, block), block)
        xf = tokens[at, :].astype(F32)
        scale = lax.rsqrt(jnp.mean(xf * xf, axis=-1, keepdims=True) + EPS)
        dn = jnp.concatenate([dn_recv[c, at, :] for c in range(pieces)], axis=1).astype(F32)
        u = dn * gain[...].astype(F32)
        inner = jnp.mean(xf * u, axis=-1, keepdims=True)
        dx = u * scale - xf * (scale * scale * scale * inner)
        out[at, :] = (d_resid + dx).astype(BF16)
        return carry

    lax.fori_loop(0, total // block, finish, 0)
    for copy in started:
        copy.wait_send()
    assert len(tags) <= send.shape[0]


def local(dp, tm, tokens, gain, w_qkv, w_out, w_pair, codebook, codes):
    patches, width = tokens.shape[2:]
    rows = w_qkv.shape[0]
    latent, n_codes = w_pair.shape[2], codebook.shape[0]
    fp = -(-tm // 8) * 8
    heads = width // HEAD_DIM
    pieces = 2
    groups = 2 if patches // tm % 32 == 0 else 1
    part_rows = patches // groups
    tags = (tm - 1) * (2 + groups + groups * pieces) + (dp - 1) + 8 * dp + 16
    vmem = pl.BlockSpec(memory_space=pltpu.VMEM)
    grad, pair, step = pl.pallas_call(
        functools.partial(kernel, (dp, tm, rows, patches, width, latent, n_codes, groups)),
        out_shape=(
            jax.ShapeDtypeStruct((patches, width), BF16),
            jax.ShapeDtypeStruct((2, latent, width), F32),
            jax.ShapeDtypeStruct((n_codes, latent), F32),
        ),
        in_specs=[vmem] * 6 + [pl.BlockSpec(memory_space=pltpu.SMEM)],
        out_specs=(vmem, vmem, vmem),
        scratch_shapes=[
            pltpu.VMEM((dp * rows, 3 * width), BF16),
            pltpu.VMEM((dp * rows, width), BF16),
            pltpu.VMEM((patches, width), BF16),
            pltpu.VMEM((patches, width), BF16),
            pltpu.VMEM((patches, 3 * width), F32),
            pltpu.VMEM((patches, 3 * width), BF16),
            pltpu.VMEM((part_rows, part_rows), F32),
            pltpu.VMEM((groups * heads, part_rows, part_rows), F32),
            pltpu.VMEM((patches, width), BF16),
            pltpu.VMEM((3, fp, width), F32),
            pltpu.VMEM((tm, 3, fp, width), F32),
            pltpu.VMEM((3, fp, width), F32),
            pltpu.VMEM((dp, 3, fp, width), F32),
            pltpu.VMEM((fp, width), F32),
            pltpu.VMEM((fp, width), BF16),
            pltpu.VMEM((patches, 3 * width), BF16),
            pltpu.VMEM((pieces, patches, width // pieces), BF16),
            pltpu.VMEM((pieces, patches, width // pieces), BF16),
            pltpu.SemaphoreType.DMA((tags,)),
            pltpu.SemaphoreType.DMA((tags,)),
            pltpu.SemaphoreType.DMA((2 + groups,)),
        ],
        compiler_params=pltpu.CompilerParams(
            collective_id=0, has_side_effects=True, vmem_limit_bytes=60 * 1024 * 1024
        ),
    )(
        tokens.reshape(patches, width), gain.reshape(1, width), w_qkv, w_out, w_pair.swapaxes(1, 2), codebook,
        codes.reshape(1, 1),
    )
    return grad.reshape(tokens.shape), pair.swapaxes(1, 2), step


def solution(mesh):
    placed = (
        P("dp", "tm", None, None),
        P(),
        P("dp", None),
        P("dp", None),
        P(),
        P(),
        P("dp", "tm", None),
    )
    return jax.shard_map(
        functools.partial(local, mesh.shape["dp"], mesh.shape["tm"]),
        mesh=mesh,
        in_specs=placed,
        out_specs=(P("dp", "tm", None, None), P(), P()),
        check_vma=False,
    )
```
